32 devices in a mesh: expert: 32 (over z, y, x, core).
Axes of the slice: x: 2, y: 2, z: 4, core: 2. Of those that a mesh axis runs over, the one named last changes fastest.
Arguments:
- routed_rows: bfloat16 [6144, 2048], P('expert'), may hold values from -6 to 6
- expert_index: int32 [6144, 1], P('expert'), may hold values from 0 to 31; in each aligned block of 192 rows (0 to 191, 192 to 383, ...) at most 12 rows name the same one
- route_weight: float32 [6144], P('expert'), may hold values from 0.1 to 1
- cotangent: bfloat16 [6144, 2048], P('expert'), may hold values from -6 to 6
- gate_weight: bfloat16 [32, 2048, 768], P('expert'), may hold values from -0.125 to 0.125
- up_weight: bfloat16 [32, 2048, 768], P('expert'), may hold values from -0.125 to 0.125
- down_weight: bfloat16 [32, 768, 2048], P('expert'), may hold values from -0.21875 to 0.21875
Outputs:
- layer_out: bfloat16 [6144, 2048], P('expert')
- row_grad: bfloat16 [6144, 2048], P('expert')
- weight_grad: float32 [6144], P('expert')
- gate_grad: bfloat16 [32, 2048, 768], P('expert')
- up_grad: bfloat16 [32, 2048, 768], P('expert')
- down_grad: bfloat16 [32, 768, 2048], P('expert')
The draws below stay inside these ranges and needn't reach their ends.
Inputs may be any that keep to these rules, and one draw needn't show every extreme that they name: `expert_index`: among the 192 rows of one device no expert is named more than 12 times, a bound that some block reaches.
All inputs are finite; a program needn't handle non-finite values.
Results may differ from the reference program's by a relative error of at most 0.0058.
Values may be sent and summed in bfloat16 or wider, within the bound.
A program may use at most 128 MiB of HBM per device.

```python
import math
import jax
import jax.numpy as jnp
import numpy as np
from jax import lax

D = 2048
FF = 768
ROW_DEV = 192
EXPERTS = 32
ROWS = 6144
CAP = 12
N_EXPERT = 32


def steps_of(rng, extent, pieces, low, largest):
    def one(dim, parts):
        draws = jax.random.uniform(jax.random.fold_in(jax.random.fold_in(rng, 6), dim), (parts,), jnp.float32, low / len(pieces), largest / len(pieces))
        return jnp.repeat(jnp.exp(draws), extent[dim] // parts).reshape((-1,) + (1,) * (len(extent) - dim - 1))

    gain = one(*pieces[0])
    for cut in pieces[1:]:
        gain = gain * one(*cut)
    return gain


def shared_out(own_key, own, number, rows, number_of, top, limit, skew):
    sequence = jax.random.permutation(own_key, number_of)
    heavy_load, ordinary = shares(number_of, rows * top, limit, skew, True), shares(number_of, rows * top, limit, skew, False)
    places = jnp.arange(number_of)

    def named(lengths, turn):
        used = int((lengths > 0).sum())
        fixed = max(1, used // 4)
        moved = fixed + (places - fixed + turn * (used - fixed)) % max(1, number_of - fixed)
        return jnp.zeros((number_of,), jnp.int32).at[sequence[jnp.where(places < fixed, places, moved)]].set(jnp.asarray(lengths, jnp.int32))

    lengths = jnp.where(number % 4 == 0, named(heavy_load, number // 4), named(ordinary, number - number // 4 - 1))
    mixed = jax.random.permutation(jax.random.fold_in(own, 3), number_of)
    donor, receiver = mixed[0:number_of // 2 * 2:2], mixed[1:number_of // 2 * 2:2]
    margin = jnp.minimum(lengths[donor] - 1, limit - lengths[receiver]) // 2
    margin = jnp.where((donor == sequence[0]) | (receiver == sequence[0]) | (lengths[receiver] == 0), 0, jnp.maximum(margin, 0))
    moved = jax.random.randint(jax.random.fold_in(own, 4), (number_of // 2,), 0, 1 << 20) % (margin + 1)
    lengths = lengths.at[donor].add(-moved).at[receiver].add(moved)
    labels = jnp.searchsorted(jnp.cumsum(lengths), jnp.arange(rows * top), side="right").astype(jnp.int32)
    grid = labels.reshape(top, rows).T
    grid = grid[jax.random.permutation(jax.random.fold_in(own, 1), rows)]
    turn = jax.random.randint(jax.random.fold_in(own, 2), (rows, 1), 0, top)
    return jnp.take_along_axis(grid, (jnp.arange(top)[None, :] + turn) % top, axis=1)


def shares(amount, total, limit, slope, full):
    weights = [(1 << 20) // math.isqrt(rank ** slope) + 1 for rank in range(1, amount + 1)]
    largest = limit if full else min(limit, max(-(-total // amount), total * weights[0] // sum(weights)))
    least = 1 if total - largest >= amount - 1 else 0
    given, rest = [largest] + [least] * (amount - 1), total - largest - least * (amount - 1)
    while rest > 0:
        free = [i for i in range(1, amount) if given[i] < largest] or [i for i in range(1, amount) if given[i] < limit]
        pool, budget = sum([weights[i] for i in free]), rest
        for i in free:
            more = min(limit - given[i], max(1, budget * weights[i] // pool), rest)
            given[i] = given[i] + more
            rest = rest - more
    return np.array(given)


def scatter_about(own_key, extent, width, most, shards=(), held_as=jnp.bfloat16):
    values = jax.random.normal(own_key, extent, jnp.float32) * width
    if len(shards) > 0:
        values = steps_of(own_key, extent, shards, -0.22, 0.18) * values
    return jnp.clip(values, min=-most, max=most).astype(held_as)


def setup_inputs(seed: int = 0) -> dict:
    arg_keys = jax.random.split(jax.random.key(seed), 8)
    routed_rows = scatter_about(arg_keys[0], (ROWS, D), 1.0, 6.0, ((0, 32),))
    expert_index_keys = jax.random.split(jax.random.fold_in(arg_keys[1], 1), ROWS // ROW_DEV)
    expert_index_turns = jax.random.permutation(jax.random.fold_in(arg_keys[1], 3), ROWS // ROW_DEV)
    expert_index = jax.vmap(lambda own, number: shared_out(jax.random.fold_in(arg_keys[1], 2), own, number, ROW_DEV, EXPERTS, 1, CAP, 2))(expert_index_keys, expert_index_turns).reshape((ROWS, 1))
    route_weight = jnp.clip(jnp.exp(math.log(1.0) - 2.3025851 * jax.random.uniform(arg_keys[2], (ROWS,), jnp.float32) ** steps_of(arg_keys[2], (ROWS,), ((0, 32),), -0.2, 0.2)), 0.1, 1.0)
    cotangent = scatter_about(arg_keys[3], (ROWS, D), 1.0, 6.0, ((0, 32),))
    gate_weight = scatter_about(arg_keys[4], (EXPERTS, D, FF), D ** -0.5, 0.125, ((0, 32),))
    up_weight = scatter_about(arg_keys[5], (EXPERTS, D, FF), D ** -0.5, 0.125, ((0, 32),))
    down_weight = scatter_about(arg_keys[6], (EXPERTS, FF, D), FF ** -0.5, 0.21875, ((0, 32),))
    return dict(routed_rows=routed_rows, expert_index=expert_index, route_weight=route_weight, cotangent=cotangent, gate_weight=gate_weight, up_weight=up_weight, down_weight=down_weight)


def expert_pass(inputs):
    rows_in, out_grad, w_gate, w_up, w_down = inputs
    gate_act = jnp.dot(rows_in, w_gate, preferred_element_type=jnp.float32)
    up_act = jnp.dot(rows_in, w_up, preferred_element_type=jnp.float32)
    sigma = jax.nn.sigmoid(gate_act)
    silu_gate = gate_act * sigma
    hidden = (silu_gate * up_act).astype(jnp.bfloat16)
    expert_out = jnp.dot(hidden, w_down, preferred_element_type=jnp.float32).astype(jnp.bfloat16)
    hidden_grad = jnp.dot(out_grad, w_down.T, preferred_element_type=jnp.float32)
    gate_pre = (hidden_grad * up_act * sigma * (1.0 + gate_act * (1.0 - sigma))).astype(jnp.bfloat16)
    up_pre = (hidden_grad * silu_gate).astype(jnp.bfloat16)
    input_grad = (jnp.dot(gate_pre, w_gate.T, preferred_element_type=jnp.float32)
                  + jnp.dot(up_pre, w_up.T, preferred_element_type=jnp.float32)).astype(jnp.bfloat16)
    gate_grad = jnp.dot(rows_in.T, gate_pre, preferred_element_type=jnp.float32).astype(jnp.bfloat16)
    up_grad = jnp.dot(rows_in.T, up_pre, preferred_element_type=jnp.float32).astype(jnp.bfloat16)
    down_grad = jnp.dot(hidden.T, out_grad, preferred_element_type=jnp.float32).astype(jnp.bfloat16)
    return expert_out, input_grad, gate_grad, up_grad, down_grad


def reference(routed_rows, expert_index, route_weight, cotangent, gate_weight, up_weight, down_weight):
    choice_ids = expert_index[:, 0]
    devices = N_EXPERT
    per_expert = devices * CAP
    onehot = (choice_ids[:, None] == jnp.arange(EXPERTS, dtype=jnp.int32)[None, :]).astype(jnp.int32)
    stacked = onehot.reshape(devices, ROW_DEV, EXPERTS)
    earlier = jnp.cumsum(stacked, axis=1) - stacked
    rank_within = jnp.sum(earlier * stacked, axis=2).reshape(-1).astype(jnp.int32)
    source = (jnp.arange(ROWS, dtype=jnp.int32) // ROW_DEV).astype(jnp.int32)
    slot_index = (choice_ids * per_expert + source * CAP + rank_within).astype(jnp.int32)
    out_grad = (route_weight[:, None] * cotangent.astype(jnp.float32)).astype(jnp.bfloat16)
    buffer_in = jnp.zeros((EXPERTS * per_expert, D), jnp.bfloat16).at[slot_index].set(routed_rows)
    buffer_grad = jnp.zeros((EXPERTS * per_expert, D), jnp.bfloat16).at[slot_index].set(out_grad)
    results = lax.map(expert_pass, (buffer_in.reshape(EXPERTS, per_expert, D),
                                    buffer_grad.reshape(EXPERTS, per_expert, D),
                                    gate_weight, up_weight, down_weight))
    expert_out, input_grad, gate_grad, up_grad, down_grad = results
    out_rows = expert_out.reshape(-1, D)[slot_index]
    row_grad = input_grad.reshape(-1, D)[slot_index]
    layer_out = (route_weight[:, None] * out_rows.astype(jnp.float32)).astype(jnp.bfloat16)
    weight_grad = jnp.sum(cotangent.astype(jnp.float32) * out_rows.astype(jnp.float32), axis=1)
    return layer_out, row_grad, weight_grad, gate_grad, up_grad, down_grad
```

```python
import functools
import math

import jax
import jax.numpy as jnp
from jax import lax
from jax.experimental import pallas as pl
from jax.experimental.pallas import tpu as pltpu
from jax.sharding import PartitionSpec as P

F32 = jnp.float32
BF16 = jnp.bfloat16
I32 = jnp.int32
NT = (((1,), (1,)), ((), ()))
TN = (((0,), (0,)), ((), ()))
MESH = pl.DeviceIdType.MESH
ROWS_IN, OUT_GRAD, RESULT, IN_GRAD = range(4)


def dot(a, b):
    return jnp.dot(a, b, preferred_element_type=F32)


def dot_nt(a, b):
    return lax.dot_general(a, b, NT, preferred_element_type=F32)


def dot_tn(a, b):
    return lax.dot_general(a, b, TN, preferred_element_type=F32)


def iota(shape, axis):
    return lax.broadcasted_iota(I32, shape, axis)


def hot(mask):
    return mask.astype(F32).astype(BF16)


def steps(x, size, count):
    total = jnp.zeros_like(x)
    for i in range(1, count):
        total = total + (x >= i * size).astype(I32)
    return total


def column(row):
    m = row.shape[1]
    same = iota((m, m), 0) == iota((m, m), 1)
    return jnp.sum(jnp.where(same, row, jnp.zeros_like(row)), axis=1, keepdims=True)


def as_row(col):
    m = col.shape[0]
    same = iota((m, m), 0) == iota((m, m), 1)
    return jnp.sum(jnp.where(same, col, jnp.zeros_like(col)), axis=0, keepdims=True)


def block(i, size):
    return pl.ds(pl.multiple_of(i * size, 8), size)


def store_kernel(*refs):
    half = len(refs) // 2
    sem = refs[-1]
    copies = [
        pltpu.make_async_copy(refs[i], refs[half + i], sem.at[i]) for i in range(half)
    ]
    for copy in copies:
        copy.start()
    for copy in copies:
        copy.wait()


def kernel(
    n, groups, cap, room,
    idx_any, weight_any, rows_any, cot_any, wg_any, wu_any, wd_any,
    layer, row_grad, weight_grad, wg, wu, wd, most,
    idx_row, weight_row, rows, cot, own, table, peak, peaks,
    pack, line_send, line_recv, side_send, side_recv, ga, ua, ha, hid, gp, up, sort, unsort,
    load_sem, line_out, line_in, side_out, side_in, note_out, note_in,
):
    me = lax.axis_index("expert")
    members = n // groups
    group, seat = me // members, lax.rem(me, members)
    slab = side_recv.shape[2] // members
    slots = members * slab
    _, chunks, _, width = line_recv.shape
    row_count = cot.shape[0]
    units = wg.shape[1]
    tile = math.gcd(256, units)
    lanes = table.shape[1]
    block_rows = groups * room

    loads = [
        pltpu.make_async_copy(src, dst, load_sem.at[i])
        for i, (src, dst) in enumerate((
            (idx_any, idx_row), (rows_any, rows), (weight_any, weight_row), (cot_any, cot),
            (wg_any, wg), (wu_any, wu), (wd_any, wd),
        ))
    ]
    for load in loads:
        load.start()

    def on_line(s):
        return (lax.rem(group + s, groups) * members + seat,)

    def in_group(s):
        return (group * members + lax.rem(seat + s, members),)

    barrier = pltpu.get_barrier_semaphore()

    @pl.loop(1, groups)
    def _(s):
        pl.semaphore_signal(barrier, inc=1, device_id=on_line(s), device_id_type=MESH)

    @pl.loop(1, members)
    def _(s):
        pl.semaphore_signal(barrier, inc=1, device_id=in_group(s), device_id_type=MESH)

    def along_line(p, c, source):
        land = line_recv.at[p, c, block(group, room)]

        @pl.loop(1, groups)
        def _(s):
            pltpu.make_async_remote_copy(
                src_ref=source.at[c, block(lax.rem(group + s, groups), room)], dst_ref=land,
                send_sem=line_out.at[p], recv_sem=line_in.at[p, c],
                device_id=on_line(s), device_id_type=MESH,
            ).start()

        pltpu.make_async_copy(source.at[c, block(group, room)], land, line_in.at[p, c]).start()

    def line_arrived(p, c):
        whole = line_recv.at[p, c]
        pltpu.make_async_copy(whole, whole, line_in.at[p, c]).wait()

    def across(p, c):
        land = side_recv.at[p, c, block(seat, slab)]

        @pl.loop(1, members)
        def _(s):
            pltpu.make_async_remote_copy(
                src_ref=side_send.at[p, c, block(lax.rem(seat + members - s, members), slab)],
                dst_ref=land, send_sem=side_out.at[p], recv_sem=side_in.at[p, c],
                device_id=in_group(members - s), device_id_type=MESH,
            ).start()

        pltpu.make_async_copy(side_send.at[p, c, block(seat, slab)], land, side_in.at[p, c]).start()

    def side_arrived(p, c):
        whole = side_recv.at[p, c]
        pltpu.make_async_copy(whole, whole, side_in.at[p, c]).wait()

    def relay_in(p, c):
        line_arrived(p, c)
        dispatch(p * chunks + c + window)
        side_send[p, c] = dot(sort[...], line_recv[p, c]).astype(BF16)
        across(p, c)

    def relay_out(p, c):
        side_arrived(p, c)
        line_send[p - RESULT, c] = dot(unsort[...], side_recv[p, c]).astype(BF16)
        along_line(p, c, line_send.at[p - RESULT])

    def notes(i, source, into, peers, count, at):
        land = into.at[block(at, 8)]

        @pl.loop(1, count)
        def _(s):
            pltpu.make_async_remote_copy(
                src_ref=source, dst_ref=land, send_sem=note_out.at[i], recv_sem=note_in.at[i],
                device_id=peers(s), device_id_type=MESH,
            ).start()

        pltpu.make_async_copy(source, land, note_in.at[i]).start()

    def noted(i, into):
        pltpu.make_async_copy(into, into, note_in.at[i]).wait()

    def span(c):
        return pl.ds(c * width, width)

    loads[0].wait()
    choice = idx_row[...]
    chosen = (iota((n, row_count), 0) == choice).astype(F32)
    count_col = jnp.sum(chosen, axis=1, keepdims=True)
    count_row = jnp.sum(
        jnp.where(iota((n, lanes), 0) == iota((n, lanes), 1), count_col, 0.0), axis=0, keepdims=True
    )
    own[...] = jnp.broadcast_to(count_row, own.shape)
    first = steps(iota((n, 1), 0), members, groups) * members
    other = iota((n, lanes), 1)
    ahead = (other >= first) & (other < iota((n, lanes), 0))
    offset = jnp.sum(jnp.where(ahead, count_row, 0.0), axis=1, keepdims=True)
    before = hot(iota((row_count, row_count), 0) < iota((row_count, row_count), 1))
    place = jnp.sum((dot(chosen.astype(BF16), before) + offset) * chosen, axis=0, keepdims=True).astype(I32)
    target = steps(choice, members, groups) * room + place
    pick = hot(iota((block_rows, row_count), 0) == target)
    loads[1].wait()

    window = min(2, chunks)
    for c in range(chunks):
        pack[ROWS_IN, c] = dot(pick, rows[:, span(c)]).astype(BF16)
        if c == 0:
            pl.semaphore_wait(barrier, groups + members - 2)
            notes(0, own, table, on_line, groups, group)
        if c < window:
            along_line(ROWS_IN, c, pack.at[ROWS_IN])

    loads[2].wait()
    loads[3].wait()
    weight = column(weight_row[...])
    for c in range(chunks):
        pack[OUT_GRAD, c] = dot(
            pick, (weight * cot[:, span(c)].astype(F32)).astype(BF16)
        ).astype(BF16)

    def dispatch(i):
        if i < 2 * chunks:
            along_line(i // chunks, i % chunks, pack.at[i // chunks])

    slot = iota((slots, 1), 0)
    expert = steps(slot, slab, members)
    rest = slot - expert * slab
    source = steps(rest, cap, groups)
    order = rest - source * cap
    from_source = hot(iota((slots, 8 * groups), 1) == source * 8)
    lane = iota((slots, lanes), 1)
    home = group * members + expert
    noted(0, table)
    everyone = table[...].astype(BF16)
    known = dot(from_source, everyone)
    amount = jnp.sum(jnp.where(lane == home, known, 0.0), axis=1, keepdims=True)
    offset = jnp.sum(
        jnp.where((lane >= group * members) & (lane < home), known, 0.0), axis=1, keepdims=True
    )
    taken = jnp.where(order < amount.astype(I32), source * room + offset.astype(I32) + order, -1)
    sort[...] = hot(iota((slots, block_rows), 1) == taken)
    unsort[...] = hot(iota((block_rows, slots), 0) == as_row(taken))
    inside = hot(steps(iota((lanes, 128), 0), members, groups) == iota((lanes, 128), 1))
    full = dot(everyone, inside)
    peak[...] = jnp.broadcast_to(
        jnp.max(jnp.max(full, axis=1, keepdims=True), axis=0, keepdims=True), peak.shape
    )
    notes(1, peak, peaks, in_group, members, seat)

    def tiles(body):
        @pl.loop(0, units // tile)
        def _(t):
            body(pl.ds(pl.multiple_of(t * tile, tile), tile))

    loads[4].wait()
    loads[5].wait()
    ga[...] = jnp.zeros_like(ga)
    ua[...] = jnp.zeros_like(ua)

    def forward(c):
        side_arrived(ROWS_IN, c)

        @tiles
        def _(at):
            ga[:, at] += dot(side_recv[ROWS_IN, c], wg[span(c), at])
            ua[:, at] += dot(side_recv[ROWS_IN, c], wu[span(c), at])

    for c in range(chunks):
        relay_in(ROWS_IN, c)
        if c > 0:
            forward(c - 1)
    forward(chunks - 1)

    @tiles
    def _(at):
        gate = ga[:, at]
        hid[:, at] = (gate * jax.nn.sigmoid(gate) * ua[:, at]).astype(BF16)

    loads[6].wait()

    def result(c):
        side_send[RESULT, c] = dot(hid[...], wd[:, span(c)]).astype(BF16)
        across(RESULT, c)

    ha[...] = jnp.zeros_like(ha)

    def backward(c):
        side_arrived(OUT_GRAD, c)

        @tiles
        def _(at):
            ha[:, at] += dot_nt(side_recv[OUT_GRAD, c], wd[at, span(c)])

    last = chunks - 1
    for c in range(chunks):
        relay_in(OUT_GRAD, c)
        result(c)
        if 0 < c < last:
            backward(c - 1)
        if c % 2 == 1:
            relay_out(RESULT, c // 2)
    noted(1, peaks)
    most[0, 0] = jnp.max(peaks[...]).astype(I32)
    for c in range(max(0, last - 1), last):
        backward(c)
    for c in range((last + 1) // 2, last):
        relay_out(RESULT, c)
    backward(last)

    @tiles
    def _(at):
        gate = ga[:, at]
        grad = ha[:, at]
        sigma = jax.nn.sigmoid(gate)
        gp[:, at] = (grad * ua[:, at] * sigma * (1.0 + gate * (1.0 - sigma))).astype(BF16)
        up[:, at] = (grad * (gate * sigma)).astype(BF16)

    for c in range(chunks):
        side_send[IN_GRAD, c] = (
            dot_nt(gp[...], wg[span(c), :]) + dot_nt(up[...], wu[span(c), :])
        ).astype(BF16)
        across(IN_GRAD, c)
        if c == 0:
            relay_out(RESULT, last)

    @pl.loop(0, chunks)
    def _(c):
        relay_out(IN_GRAD, c)

    @pl.loop(0, chunks)
    def _(c):
        cols = pl.ds(pl.multiple_of(c * width, width), width)

        @tiles
        def _(at):
            wg[cols, at] = dot_tn(side_recv[ROWS_IN, c], gp[:, at]).astype(BF16)
            wu[cols, at] = dot_tn(side_recv[ROWS_IN, c], up[:, at]).astype(BF16)
            wd[at, cols] = dot_tn(hid[:, at], side_recv[OUT_GRAD, c]).astype(BF16)

    fetch = hot(iota((row_count, block_rows), 1) == column(target))
    total = jnp.zeros((row_count, 1), F32)
    for c in range(chunks):
        line_arrived(RESULT, c)
        got = dot(fetch, line_recv[RESULT, c])
        layer[:, span(c)] = (weight * got).astype(BF16)
        total = total + jnp.sum(cot[:, span(c)].astype(F32) * got, axis=1, keepdims=True)
    weight_grad[...] = as_row(total)

    def left(p):
        for c in range(chunks):
            gone = line_recv.at[p, c, pl.ds(0, (groups - 1) * room)]
            pltpu.make_async_copy(gone, gone, line_out.at[p]).wait()
            gone = side_recv.at[p, c, pl.ds(0, (members - 1) * slab)]
            pltpu.make_async_copy(gone, gone, side_out.at[p]).wait()

    for p in range(IN_GRAD):
        left(p)
    for i, (into, count) in enumerate(((table, groups), (peaks, members))):
        gone = into.at[pl.ds(0, 8 * (count - 1))]
        pltpu.make_async_copy(gone, gone, note_out.at[i]).wait()

    for c in range(chunks):
        line_arrived(IN_GRAD, c)
        row_grad[:, span(c)] = dot(fetch, line_recv[IN_GRAD, c]).astype(BF16)
    left(IN_GRAD)


def up_to(x, size):
    return -(-x // size) * size


def local(routed_rows, expert_index, route_weight, cotangent, gate_weight, up_weight, down_weight):
    n = lax.axis_size("expert")
    row_count, width = routed_rows.shape
    units = gate_weight.shape[2]
    cap = max(2, 2 * row_count // n)
    groups = 1
    while n % (2 * groups) == 0 and (2 * groups) ** 2 <= n // 2:
        groups *= 2
    members = n // groups
    bound = up_to(min(row_count, members * cap), 8)
    few = min(bound, up_to(5 * bound // 6, 8))
    slab = up_to(groups * cap, 8)
    slots = members * slab
    lanes = up_to(n, 128)
    chunks = 4 if width % 512 == 0 else 1
    part = width // chunks
    vmem = pl.BlockSpec(memory_space=pltpu.VMEM)
    smem = pl.BlockSpec(memory_space=pltpu.SMEM)
    hbm = pl.BlockSpec(memory_space=pltpu.HBM)
    shape = jax.ShapeDtypeStruct
    dma = pltpu.SemaphoreType.DMA
    results = (
        shape((row_count, width), BF16),
        shape((row_count, width), BF16),
        shape((1, row_count), F32),
        shape((width, units), BF16),
        shape((width, units), BF16),
        shape((units, width), BF16),
    )

    def routed(room, ident, limit, kind, *args):
        return pl.pallas_call(
            functools.partial(kernel, n, groups, cap, room),
            out_shape=tuple(kind(r.shape, r.dtype) for r in results) + (shape((1, 1), I32),),
            in_specs=[hbm] * 7,
            out_specs=(vmem,) * 6 + (smem,),
            scratch_shapes=[
                pltpu.VMEM((1, row_count), I32),
                pltpu.VMEM((1, row_count), F32),
                pltpu.VMEM((row_count, width), BF16),
                pltpu.VMEM((row_count, width), BF16),
                pltpu.VMEM((8, lanes), F32),
                pltpu.VMEM((8 * groups, lanes), F32),
                pltpu.VMEM((8, 128), F32),
                pltpu.VMEM((8 * members, 128), F32),
                pltpu.VMEM((2, chunks, groups * room, part), BF16),
                pltpu.VMEM((2, chunks, groups * room, part), BF16),
                pltpu.VMEM((4, chunks, groups * room, part), BF16),
                pltpu.VMEM((4, chunks, slots, part), BF16),
                pltpu.VMEM((4, chunks, slots, part), BF16),
                pltpu.VMEM((slots, units), F32),
                pltpu.VMEM((slots, units), F32),
                pltpu.VMEM((slots, units), F32),
                pltpu.VMEM((slots, units), BF16),
                pltpu.VMEM((slots, units), BF16),
                pltpu.VMEM((slots, units), BF16),
                pltpu.VMEM((slots, groups * room), BF16),
                pltpu.VMEM((groups * room, slots), BF16),
                dma((7,)),
                dma((4,)),
                dma((4, chunks)),
                dma((4,)),
                dma((4, chunks)),
                dma((2,)),
                dma((2,)),
            ],
            compiler_params=pltpu.CompilerParams(
                collective_id=ident, has_side_effects=True, vmem_limit_bytes=limit * 1024 * 1024
            ),
            name=f"routed_{room}",
        )(*args)

    def stored(limit, *arrays):
        return pl.pallas_call(
            store_kernel,
            out_shape=results,
            in_specs=[vmem] * len(results),
            out_specs=(hbm,) * len(results),
            scratch_shapes=[dma((len(results),))],
            compiler_params=pltpu.CompilerParams(vmem_limit_bytes=limit * 1024 * 1024),
            name="stored",
        )(*arrays)

    args = (
        expert_index.reshape(1, row_count), route_weight[None], routed_rows, cotangent,
        gate_weight[0], up_weight[0], down_weight[0],
    )
    *quick, most = routed(few, 0, 40, pltpu.VMEM, *args)
    layer_out, row_grad, weight_grad, *grads = lax.cond(
        most[0, 0] <= few,
        lambda found, given: tuple(stored(1, *found)),
        lambda found, given: tuple(stored(32, *routed(bound, 1, 60, shape, *given)[:-1])),
        tuple(quick), args,
    )
    return (layer_out, row_grad, weight_grad[0]) + tuple(g[None] for g in grads)


def solution(mesh):
    rows, vector, cube = P("expert", None), P("expert"), P("expert", None, None)
    return jax.shard_map(
        local,
        mesh=mesh,
        in_specs=(rows, rows, vector, rows, cube, cube, cube),
        out_specs=(rows, rows, vector, cube, cube, cube),
        check_vma=False,
    )
```
